32 devices in a mesh: seq: 16 (over z, y, x), head: 2 (over core).
Axes of the slice: x: 2, y: 2, z: 4, core: 2. Of those that a mesh axis runs over, the one named last changes fastest.
Arguments:
- queries: bfloat16 [4096, 64, 192], P('seq', 'head'), may hold values from -50 to 50
- grad_out: bfloat16 [4096, 64, 128], P('seq', 'head'), may hold values from -6 to 6
- latent: bfloat16 [4096, 576], P('seq'), may hold values from -18 to 18
- w_uk: bfloat16 [64, 512, 128], P('head'), may hold values from -0.25 to 0.25
- w_uv: bfloat16 [64, 512, 128], P('head'), may hold values from -0.25 to 0.25
- doc_start: int32 [4096], P('seq'), may hold values from 0 to 4095, as said below
Outputs:
- grad_query: bfloat16 [4096, 64, 192], P('seq', 'head')
- grad_latent: float32 [4096, 576], P(('seq', 'head'))
The draws below stay inside these ranges and needn't reach their ends.
Inputs may be any that keep to these rules, and one draw needn't show every extreme that they name: doc_start[t] is the first position of the document that holds position t; documents follow one another, each of 1 to 768 positions, and one is exactly 768 long.
All inputs are finite; a program needn't handle non-finite values.
Results may differ from the reference program's by a relative error of at most 0.008.
Values may be sent and summed in bfloat16 or wider, within the bound.
A program may use at most 192 MiB of HBM per device.

```python
import jax
import jax.numpy as jnp
from jax import lax

HEADS = 64
NOPE = 128
ROPE = 64
LATENT = 512
VDIM = 128
T_DEV = 256
BACK = 3
MOST = 768
SEQ = 4096
N_SEQ = 16


def draw_latent(key, part):
    values = jnp.clip(jax.random.normal(jax.random.fold_in(key, 11), (SEQ, LATENT + ROPE), jnp.float32), -6.0, 6.0)
    return values.astype(jnp.bfloat16)


def draw_queries(key, part):
    values = jnp.clip(jax.random.normal(jax.random.fold_in(key, 21), (SEQ, HEADS, NOPE + ROPE), jnp.float32), -6.0, 6.0)
    return values.astype(jnp.bfloat16)


def draw_doc_start(key, part):
    key_len, key_first = jax.random.split(jax.random.fold_in(key, 31))
    lengths = jax.random.randint(key_len, (SEQ,), 1, MOST + 1)
    first = jax.random.randint(key_first, (), 1, T_DEV)
    lengths = lengths.at[0].set(first).at[1].set(MOST)
    ends = jnp.cumsum(lengths).astype(jnp.int32)
    starts = (ends - lengths).astype(jnp.int32)
    position = jnp.arange(SEQ, dtype=jnp.int32)
    which = jnp.searchsorted(ends, position, side='right')
    result = starts[which].astype(jnp.int32)
    result = jnp.where(position == SEQ - 1, SEQ - 1, result)
    return result.astype(jnp.int32)


def block_levels(own_key, shape, shards, least, top_value):
    factor_of = 1.0
    for dim, blocks in shards:
        draws = jax.random.uniform(jax.random.fold_in(jax.random.fold_in(own_key, 6), dim), (blocks,), jnp.float32, least / len(shards), top_value / len(shards))
        factor_of = factor_of * jnp.repeat(jnp.exp(draws), shape[dim] // blocks).reshape((-1,) + (1,) * (len(shape) - 1 - dim))
    return factor_of


def normal_values(stream_key, dims, scale, most, cuts=(), kind=jnp.bfloat16):
    drawn = jax.random.normal(stream_key, dims, jnp.float32) * scale
    if len(cuts) > 0:
        drawn = block_levels(stream_key, dims, cuts, -0.22, 0.18) * drawn
    return jnp.clip(drawn, min=-most, max=most).astype(kind)


def setup_inputs(seed: int = 0) -> dict:
    splits = jax.random.split(jax.random.key(seed), 7)
    queries = draw_queries(jax.random.fold_in(splits[6], 71), 0)
    grad_out = normal_values(splits[1], (SEQ, HEADS, VDIM), 1.0, 6.0, ((0, 16), (1, 2)))
    latent = draw_latent(jax.random.fold_in(splits[6], 71), 0)
    w_uk = normal_values(splits[3], (HEADS, LATENT, NOPE), LATENT ** -0.5, 0.25, ((0, 2),))
    w_uv = normal_values(splits[4], (HEADS, LATENT, VDIM), LATENT ** -0.5, 0.25, ((0, 2),))
    doc_start = draw_doc_start(jax.random.fold_in(splits[6], 71), 0)
    return dict(queries=queries, grad_out=grad_out, latent=latent, w_uk=w_uk, w_uv=w_uv, doc_start=doc_start)


def rounded(values):
    return lax.optimization_barrier(values.astype(jnp.bfloat16)).astype(jnp.float32)


def reference(queries, grad_out, latent, w_uk, w_uv, doc_start):
    width = LATENT + ROPE
    factor = (NOPE + ROPE) ** -0.5
    span = (BACK + 1) * T_DEV
    front = BACK * T_DEV
    padded = jnp.concatenate([jnp.zeros((front, width), latent.dtype), latent], 0)
    uk_full = w_uk.astype(jnp.float32)
    uv_full = w_uv.astype(jnp.float32)

    def step(carry, index):
        start = (index * T_DEV).astype(jnp.int32)
        query = lax.dynamic_slice_in_dim(queries, start, T_DEV, 0).astype(jnp.float32)
        cotangent = lax.dynamic_slice_in_dim(grad_out, start, T_DEV, 0).astype(jnp.float32)
        starts = lax.dynamic_slice_in_dim(doc_start, start, T_DEV, 0)
        keys = lax.dynamic_slice_in_dim(padded, start, span, 0).astype(jnp.float32)
        qpos = start + jnp.arange(T_DEV, dtype=jnp.int32)
        kpos = start - front + jnp.arange(span, dtype=jnp.int32)
        visible = (kpos[None, :] >= starts[:, None]) & (kpos[None, :] <= qpos[:, None])
        q_abs = rounded(jnp.einsum('thn,hln->thl', query[:, :, :NOPE], uk_full))
        qcat = jnp.concatenate([q_abs, query[:, :, NOPE:]], -1)
        scores = jnp.einsum('thc,uc->htu', qcat, keys) * factor
        scores = jnp.where(visible[None], scores, -jnp.inf)
        top = jnp.max(scores, -1, keepdims=True)
        expo = jnp.exp(scores - top)
        probs = rounded(expo / jnp.sum(expo, -1, keepdims=True))
        grad_lat = rounded(jnp.einsum('thv,hlv->thl', cotangent, uv_full))
        o_lat = jnp.einsum('htu,ul->thl', probs, keys[:, :LATENT])
        delta = jnp.sum(grad_lat * o_lat, -1)
        dprob = jnp.einsum('thl,ul->htu', grad_lat, keys[:, :LATENT])
        dscore = rounded(probs * (dprob - delta.T[:, :, None]))
        dq_cat = jnp.einsum('htu,uc->thc', dscore, keys) * factor
        dq_nope = jnp.einsum('thl,hln->thn', rounded(dq_cat[:, :, :LATENT]), uk_full)
        grad_query = jnp.concatenate([dq_nope, dq_cat[:, :, LATENT:]], -1).astype(jnp.bfloat16)
        dkey = jnp.einsum('htu,thc->uc', dscore, qcat) * factor
        dvalue = jnp.einsum('htu,thl->ul', probs, grad_lat)
        dkey = dkey + jnp.pad(dvalue, ((0, 0), (0, ROPE)))
        window = lax.dynamic_slice_in_dim(carry, start, span, 0) + dkey
        carry = lax.dynamic_update_slice_in_dim(carry, window, start, 0)
        return carry, grad_query

    init = jnp.zeros((front + N_SEQ * T_DEV, width), jnp.float32)
    total, pieces = lax.scan(step, init, jnp.arange(N_SEQ, dtype=jnp.int32))
    return pieces.reshape(N_SEQ * T_DEV, HEADS, NOPE + ROPE), total[front:]
```

```python
import functools
import math

import jax
import jax.numpy as jnp
from jax import lax
from jax.experimental import pallas as pl
from jax.experimental.pallas import tpu as pltpu
from jax.sharding import PartitionSpec as P

BACK = 3
LANES = 128
STRIP = 32
HIDDEN = -1e30
F32 = jnp.float32
BF16 = jnp.bfloat16
NN = (((1,), (0,)), ((), ()))
NT = (((1,), (1,)), ((), ()))


def dot(a, b, dims=NN):
    return lax.dot_general(a, b, dims, preferred_element_type=F32)


def attend_kernel(tokens, factor, halves, sizes, count, side, starts, q_hbm, g_hbm, uk_hbm, uv_hbm, kt_ref,
                  gq_hbm, *refs):
    sums = refs[:2] if halves else refs[:1]
    (q_ref, g_ref, uk_ref, uv_ref, gq_ref, lat_ref, bias_ref, acc_ref, kv_ref, score_refs, dprob_refs,
     probs_refs, dscore_refs, dkv_refs, top_refs, inverse_refs, in_sems, out_sems) = refs[len(sums):]
    width, span = kt_ref.shape
    heads, depth, _ = q_ref.shape
    latw, nope = uk_ref.shape[1:]
    sources = [(q_hbm, q_ref), (g_hbm, g_ref), (uk_hbm, uk_ref), (uv_hbm, uv_ref)]

    def fetch(index, which):
        source, target = sources[which]
        return pltpu.make_async_copy(source.at[index], target.at[index], in_sems.at[which, index])

    def put(index):
        return pltpu.make_async_copy(gq_ref.at[index], gq_hbm.at[index], out_sems.at[index])

    def start(index, carry):
        for which in range(len(sources)):
            fetch(index, which).start()
        return carry

    lax.fori_loop(0, heads, start, 0)
    acc_ref[...] = jnp.zeros_like(acc_ref)
    for j in range(span // LANES):
        part = pl.ds(j * LANES, LANES)
        lat_ref[part, :] = kt_ref[:, part].T
        kpos = lax.broadcasted_iota(jnp.int32, (LANES, tokens), 0) + j * LANES
        qpos = lax.broadcasted_iota(jnp.int32, (LANES, tokens), 1) + (span - tokens)
        seen = (kpos >= starts[...]) & (kpos <= qpos)
        bias_ref[part, :] = jnp.where(seen, 0.0, HIDDEN)
    for slot in range(2):
        for ref in (score_refs, dprob_refs, probs_refs, dscore_refs, top_refs, inverse_refs):
            ref[slot][...] = jnp.zeros_like(ref[slot])
    kv_ref[...] = jnp.zeros_like(kv_ref)

    def run(size):
        rows = slice(span - size, span)
        chunks = [slice(r, r + STRIP) for r in range(span - size, span, STRIP)]
        trips = heads // 2 + 1

        def both(index):
            return jnp.concatenate([uk_ref[index], uv_ref[index]], 1)

        def half(trip, slot):
            turn = trip * 2 + slot
            first = jnp.minimum(turn, heads - 1)
            last = jnp.clip(turn - 2, 0, heads - 1)
            now, before = lax.rem(turn, 4), lax.rem(turn + 2, 4)
            probs, dscore = probs_refs[slot], dscore_refs[slot]
            inverse = inverse_refs[slot][...]
            kv = dot(lat_ref[rows, :latw], both(first)).astype(BF16)
            kv_ref[now, rows, :] = kv
            turned = (g_ref[last].T.astype(F32) * inverse).astype(BF16)
            dvalue = dot(probs[rows, :], turned, NT)
            query = (q_ref[last].astype(F32) * (inverse * factor)).astype(BF16)
            dkey = dot(dscore[rows, :], query, NT)
            key = jnp.concatenate([kv[:, :nope], lat_ref[rows, latw:]], 1)
            scores = dot(key, q_ref[first]) + bias_ref[rows, :]
            score_refs[slot][rows, :] = scores
            top_refs[slot][...] = jnp.max(scores, 0, keepdims=True)
            dkv_refs[slot][rows, :nope] = dkey[:, :nope].astype(BF16)
            dkv_refs[slot][rows, nope:] = dvalue.astype(BF16)
            acc_ref[rows, latw:] += dkey[:, nope:]
            if slot:
                pair = jnp.concatenate([dkv_refs[0][rows, :], dkv_refs[1][rows, :]], 1)
                other = jnp.maximum(last - 1, 0)
                weights = jnp.concatenate([both(other), both(last)], 1)
                acc_ref[rows, :latw] += dot(pair, weights, NT)
            dprob_refs[slot][rows, :] = dot(kv[:, nope:], g_ref[first], NT)
            key = jnp.concatenate([kv_ref[before, rows, :nope], lat_ref[rows, latw:]], 1)
            dq = dot(key.T, dscore[rows, :])
            gq_ref[last] = (dq * (inverse * factor)).astype(BF16)

        def normalize(slot, turn):
            score_ref, dprob_ref = score_refs[slot], dprob_refs[slot]
            probs_ref, dscore_ref = probs_refs[slot], dscore_refs[slot]
            top = top_refs[slot][...]
            total = jnp.zeros((STRIP, tokens), F32)
            delta = jnp.zeros((STRIP, tokens), F32)
            for part in chunks:
                expo = jnp.exp2((score_ref[part, :] - top) * (factor * math.log2(math.e)))
                probs_ref[part, :] = expo.astype(BF16)
                total += expo
                delta += expo * dprob_ref[part, :]
            inverse = 1.0 / jnp.sum(total, 0, keepdims=True)
            delta = jnp.sum(delta, 0, keepdims=True) * inverse
            valid = jnp.where((turn >= 0) & (turn < heads), 1.0, 0.0)
            inverse_refs[slot][...] = inverse * valid
            for part in chunks:
                expo = probs_ref[part, :].astype(F32)
                dscore_ref[part, :] = (expo * (dprob_ref[part, :] - delta)).astype(BF16)

        def step(trip, carry):
            @pl.when(trip < trips - 1)
            def _():
                for which in range(len(sources)):
                    fetch(trip * 2, which).wait()
                    fetch(trip * 2 + 1, which).wait()

            half(trip, 0)
            normalize(1, trip * 2 - 1)
            half(trip, 1)
            normalize(0, trip * 2)

            @pl.when(trip > 0)
            def _():
                put(trip * 2 - 2).start()
                put(trip * 2 - 1).start()

            return carry

        lax.fori_loop(0, trips, step, 0)

    least = 0
    for size in sizes:
        pl.when((count[0] * LANES > least) & (count[0] * LANES <= size))(functools.partial(run, size))
        least = size

    if halves:
        mine_ref, theirs_ref = sums
        half = tokens // 2
        for r in range(span // tokens):
            own = pl.ds(pl.multiple_of(r * tokens + side[0] * half, half), half)
            other = pl.ds(pl.multiple_of(r * tokens + (1 - side[0]) * half, half), half)
            mine_ref[r] = acc_ref[own, :].T
            theirs_ref[r] = acc_ref[other, :].astype(BF16).T
    else:
        for r in range(span // tokens):
            sums[0][r] = acc_ref[r * tokens:(r + 1) * tokens, :].T

    def finish(index, carry):
        put(index).wait()
        return carry

    lax.fori_loop(0, heads, finish, 0)


def attend(count, side, starts, q, g, uk, uv, keys, halves):
    heads, depth, tokens = q.shape
    latw, nope = uk.shape[1:]
    vdim = uv.shape[2]
    width, span = keys.shape
    share = tokens // 2 if halves else tokens
    sums = [F32, BF16] if halves else [F32]
    sizes = sorted({span // 2, span - 2 * LANES, span - LANES, span})
    smem = pl.BlockSpec(memory_space=pltpu.SMEM)
    vmem = pl.BlockSpec(memory_space=pltpu.VMEM)
    hbm = pl.BlockSpec(memory_space=pl.ANY)
    two = lambda shape, kind: [pltpu.VMEM(shape, kind)] * 2
    return pl.pallas_call(
        functools.partial(attend_kernel, tokens, depth ** (-0.5), halves, sizes),
        in_specs=[smem, smem, vmem, hbm, hbm, hbm, hbm, vmem],
        out_specs=[hbm] + [vmem] * len(sums),
        out_shape=[
            jax.ShapeDtypeStruct((heads, depth, tokens), BF16),
            *[jax.ShapeDtypeStruct((span // tokens, width, share), kind) for kind in sums],
        ],
        scratch_shapes=[
            pltpu.VMEM((heads, depth, tokens), BF16),
            pltpu.VMEM((heads, tokens, vdim), BF16),
            pltpu.VMEM((heads, latw, nope), BF16),
            pltpu.VMEM((heads, latw, vdim), BF16),
            pltpu.VMEM((heads, depth, tokens), BF16),
            pltpu.VMEM((span, width), BF16),
            pltpu.VMEM((span, tokens), F32),
            pltpu.VMEM((span, width), F32),
            pltpu.VMEM((4, span, nope + vdim), BF16),
            two((span, tokens), F32),
            two((span, tokens), F32),
            two((span, tokens), BF16),
            two((span, tokens), BF16),
            two((span, nope + vdim), BF16),
            two((1, tokens), F32),
            two((1, tokens), F32),
            pltpu.SemaphoreType.DMA((4, heads)),
            pltpu.SemaphoreType.DMA((heads,)),
        ],
        compiler_params=pltpu.CompilerParams(vmem_limit_bytes=60 * 1024 * 1024),
        name="attend",
    )(count, side, starts, q, g, uk, uv, keys)


def places():
    me = lax.axis_index("seq")
    count = lax.axis_size("seq")
    head = lax.axis_index("head")
    ahead = [(lax.rem(me + r, count), head) for r in range(1, BACK + 1)]
    behind = [(lax.rem(me + count - r, count), head) for r in range(1, BACK + 1)]
    return head, ahead, behind, (me, 1 - head)


def meet(peers):
    barrier = pltpu.get_barrier_semaphore()
    for peer in peers:
        pl.semaphore_signal(barrier, inc=1, device_id=peer, device_id_type=pl.DeviceIdType.MESH)
    pl.semaphore_wait(barrier, len(peers))


def send(src, dst, sems, slot, peer):
    copy = pltpu.make_async_remote_copy(
        src_ref=src, dst_ref=dst, send_sem=sems.at[0, slot], recv_sem=sems.at[1, slot],
        device_id=peer, device_id_type=pl.DeviceIdType.MESH,
    )
    copy.start()
    return copy


def gather_kernel(own_ref, keys_ref, far_sems, near_sems):
    tokens = own_ref.shape[1]
    half = tokens // 2
    head, ahead, behind, sibling = places()
    meet(ahead + behind + [sibling])
    mine = pl.ds(pl.multiple_of(head * half, half), half)
    landing = [
        keys_ref.at[:, pl.ds(pl.multiple_of((BACK - r) * tokens + head * half, half), half)]
        for r in range(1, BACK + 1)
    ]
    far = [send(own_ref.at[:, mine], landing[r], far_sems, r, ahead[r]) for r in range(BACK)]
    keys_ref[:, BACK * tokens:] = own_ref[...]
    near = []
    for r in range(BACK):
        far[r].wait_recv()
        near.append(send(landing[r], landing[r], near_sems, r, sibling))
    for r in range(BACK):
        far[r].wait_send()
        near[r].wait()


def gather(own):
    width, tokens = own.shape
    return pl.pallas_call(
        gather_kernel,
        out_shape=jax.ShapeDtypeStruct((width, (BACK + 1) * tokens), own.dtype),
        in_specs=[pl.BlockSpec(memory_space=pltpu.VMEM)],
        out_specs=pl.BlockSpec(memory_space=pltpu.VMEM),
        scratch_shapes=[pltpu.SemaphoreType.DMA((2, BACK)), pltpu.SemaphoreType.DMA((2, BACK))],
        compiler_params=pltpu.CompilerParams(collective_id=0, has_side_effects=True),
        name="gather",
    )(own)


def combine_kernel(mine_ref, theirs_ref, out_ref, near_ref, part_ref, far_ref, near_sems, far_sems):
    _, ahead, behind, sibling = places()
    meet(ahead + behind + [sibling])
    near = [
        send(theirs_ref.at[r], near_ref.at[r], near_sems, r, sibling) for r in range(BACK + 1)
    ]
    far = []
    for r in range(BACK):
        near[r].wait_recv()
        part_ref[r] = (mine_ref[r] + near_ref[r].astype(F32)).astype(BF16)
        far.append(send(part_ref.at[r], far_ref.at[r], far_sems, r, behind[BACK - 1 - r]))
    near[BACK].wait_recv()
    out_ref[...] = mine_ref[BACK] + near_ref[BACK].astype(F32)
    for r in range(BACK):
        far[r].wait_recv()
        out_ref[...] += far_ref[r].astype(F32)
    for r in range(BACK + 1):
        near[r].wait_send()
    for r in range(BACK):
        far[r].wait_send()


def combine(mine, theirs):
    shape = mine.shape[1:]
    return pl.pallas_call(
        combine_kernel,
        out_shape=jax.ShapeDtypeStruct(shape, F32),
        in_specs=[pl.BlockSpec(memory_space=pltpu.VMEM)] * 2,
        out_specs=pl.BlockSpec(memory_space=pltpu.VMEM),
        scratch_shapes=[
            pltpu.VMEM((BACK + 1,) + shape, BF16),
            pltpu.VMEM((BACK,) + shape, BF16),
            pltpu.VMEM((BACK,) + shape, BF16),
            pltpu.SemaphoreType.DMA((2, BACK + 1)),
            pltpu.SemaphoreType.DMA((2, BACK)),
        ],
        compiler_params=pltpu.CompilerParams(collective_id=1, has_side_effects=True),
        name="combine",
    )(mine, theirs)


def shift(block, axis, distance):
    devices = range(lax.axis_size(axis))
    route = [(i - distance, i) for i in devices if i - distance in devices]
    return lax.ppermute(block, axis, route)


def shards(queries, grad_out, latent, w_uk, w_uv, doc_start):
    tokens, heads, depth = queries.shape
    span = (BACK + 1) * tokens
    own = latent.T
    halves = lax.axis_size("head") == 2
    if halves:
        keys = gather(own)
    else:
        received = [shift(own, "seq", level) for level in range(BACK, 0, -1)]
        keys = jnp.concatenate(received + [own], 1)
    starts = doc_start - (lax.axis_index("seq") - BACK) * tokens
    count = span // LANES - starts[:1] // LANES
    side = lax.axis_index("head").astype(jnp.int32)[None]
    grad_q, mine, *theirs = attend(
        count,
        side,
        starts[None, :],
        queries.transpose(1, 2, 0),
        grad_out.transpose(1, 0, 2),
        w_uk,
        w_uv,
        keys,
        halves,
    )
    grad_query = grad_q.transpose(2, 0, 1)
    if halves:
        return grad_query, combine(mine, theirs[0]).T
    back = [shift(mine[BACK - r].astype(BF16), "seq", -r) for r in range(1, BACK + 1)]
    total = mine[BACK]
    for piece in back:
        total = total + piece.astype(F32)
    return grad_query, lax.psum_scatter(total.T, "head", scatter_dimension=0, tiled=True)


def solution(mesh):
    placed = (
        P("seq", "head", None),
        P("seq", "head", None),
        P("seq", None),
        P("head", None, None),
        P("head", None, None),
        P("seq"),
    )
    return jax.shard_map(
        shards,
        mesh=mesh,
        in_specs=placed,
        out_specs=(P("seq", "head", None), P(("seq", "head"), None)),
        check_vma=False,
    )
```

```python
import functools
import math

import jax
import jax.numpy as jnp
from jax import lax
from jax.experimental import pallas as pl
from jax.experimental.pallas import tpu as pltpu
from jax.sharding import PartitionSpec as P

BACK = 3
LANES = 128
STRIP = 32
RING = 3
MANY = 4
DEEP = 16
HIDDEN = -1e30
F32 = jnp.float32
BF16 = jnp.bfloat16
NN = (((1,), (0,)), ((), ()))
NT = (((1,), (1,)), ((), ()))


def dot(a, b, dims=NN):
    return lax.dot_general(a, b, dims, preferred_element_type=F32)


def attend_kernel(tokens, factor, sizes, count, starts, rope_ref, q_hbm, g_hbm, kv_hbm,
                  gq_hbm, dkv_hbm, turned_ref, q_ref, g_ref, gq_ref, kv_ref, dkv_ref, zero_ref, bias_ref, acc_ref,
                  score_refs, dprob_refs, probs_refs, dscore_refs, top_refs, inverse_refs,
                  in_sems, kv_sems, dkv_sems, zero_sems, out_sems):
    span, rope = rope_ref.shape
    heads, depth, _ = q_ref.shape
    nope = depth - rope
    trips = heads // 2 + 1
    groups = heads // MANY
    sources = [(q_hbm, q_ref), (g_hbm, g_ref)]

    def fetch(group, which):
        source, target = sources[which]
        some = pl.ds(group * MANY, MANY)
        return pltpu.make_async_copy(source.at[some], target.at[some], in_sems.at[which, group])

    def put(pair):
        some = pl.ds(pair * 2, 2)
        return pltpu.make_async_copy(gq_ref.at[some], gq_hbm.at[some], out_sems.at[pair])

    def run(size):
        rows = slice(span - size, span)
        chunks = [slice(r, r + STRIP) for r in range(span - size, span, STRIP)]

        def load(pair, size=size):
            slot = lax.rem(pair, RING)
            return pltpu.make_async_copy(
                kv_hbm.at[pl.ds(pair * 2, 2), pl.ds(span - size, size)],
                kv_ref.at[slot, :, pl.ds(span - size, size)],
                kv_sems.at[slot],
            )

        def save(pair):
            slot = lax.rem(pair, 2)
            return pltpu.make_async_copy(
                dkv_ref.at[slot, :, pl.ds(0, size)],
                dkv_hbm.at[pl.ds(pair * 2, 2), pl.ds(span - size, size)],
                dkv_sems.at[slot],
            )

        def clear(group):
            return pltpu.make_async_copy(
                zero_ref.at[:, pl.ds(0, span - size)],
                dkv_hbm.at[pl.ds(group * MANY, MANY), pl.ds(0, span - size)],
                zero_sems.at[group],
            )

        def half(trip, slot):
            turn = trip * 2 + slot
            first = jnp.minimum(turn, heads - 1)
            last = jnp.clip(turn - 2, 0, heads - 1)
            now = lax.rem(jnp.minimum(trip, trips - 2), RING)
            before = lax.rem(jnp.maximum(trip - 1, 0), RING)
            probs, dscore = probs_refs[slot], dscore_refs[slot]
            inverse = inverse_refs[slot][...]
            turned = (g_ref[last].T.astype(F32) * inverse).astype(BF16)
            query = (q_ref[last].astype(F32) * (inverse * factor)).astype(BF16)
            dvalue = dot(probs[rows, :], turned, NT)
            dkey = dot(dscore[rows, :], query, NT)
            place = lax.rem(trip + 1, 2)
            dkv_ref[place, slot, :size, nope:] = dvalue.astype(BF16)
            dkv_ref[place, slot, :size, :nope] = dkey[:, :nope].astype(BF16)
            acc_ref[rows, :] += dkey[:, nope:]
            key = jnp.concatenate([kv_ref[now, slot, rows, :nope], rope_ref[rows, :]], 1)
            scores = dot(key, q_ref[first]) + bias_ref[rows, :]
            score_refs[slot][rows, :] = scores
            top_refs[slot][...] = jnp.max(scores, 0, keepdims=True)
            dprob_refs[slot][rows, :] = dot(kv_ref[now, slot, rows, nope:], g_ref[first], NT)
            key = jnp.concatenate([kv_ref[before, slot, rows, :nope], rope_ref[rows, :]], 1)
            dq = dot(key.T, dscore[rows, :])
            gq_ref[last] = (dq * (inverse * factor)).astype(BF16)

        def normalize(slot, turn):
            score_ref, dprob_ref = score_refs[slot], dprob_refs[slot]
            probs_ref, dscore_ref = probs_refs[slot], dscore_refs[slot]
            top = top_refs[slot][...]
            total = jnp.zeros((STRIP, tokens), F32)
            delta = jnp.zeros((STRIP, tokens), F32)
            for part in chunks:
                expo = jnp.exp2((score_ref[part, :] - top) * (factor * math.log2(math.e)))
                probs_ref[part, :] = expo.astype(BF16)
                total += expo
                delta += expo * dprob_ref[part, :]
            inverse = 1.0 / jnp.sum(total, 0, keepdims=True)
            delta = jnp.sum(delta, 0, keepdims=True) * inverse
            valid = jnp.where((turn >= 0) & (turn < heads), 1.0, 0.0)
            inverse_refs[slot][...] = inverse * valid
            for part in chunks:
                expo = probs_ref[part, :].astype(F32)
                dscore_ref[part, :] = (expo * (dprob_ref[part, :] - delta)).astype(BF16)

        def step(trip, carry):
            @pl.when((lax.rem(trip, MANY // 2) == 0) & (trip < trips - 1))
            def _():
                fetch(lax.div(trip, MANY // 2), 0).wait()
                fetch(lax.div(trip, MANY // 2), 1).wait()

            @pl.when((trip > 0) & (trip < trips - 1))
            def _():
                load(trip).wait()

            @pl.when(trip < trips - 2)
            def _():
                load(trip + 1).start()

            @pl.when(trip > 2)
            def _():
                save(trip - 3).wait()

            half(trip, 0)
            normalize(1, trip * 2 - 1)
            half(trip, 1)
            normalize(0, trip * 2)

            @pl.when(trip > 0)
            def _():
                put(trip - 1).start()
                save(trip - 1).start()

            return carry

        if size < span:
            for group in range(groups):
                clear(group).start()
        prime.wait()
        lax.fori_loop(0, trips, step, 0)
        for pair in range(max(trips - 3, 0), trips - 1):
            save(pair).wait()
        if size < span:
            for group in range(groups):
                clear(group).wait()

    prime = pltpu.make_async_copy(kv_hbm.at[pl.ds(0, 2)], kv_ref.at[0], kv_sems.at[0])
    prime.start()
    for group in range(groups):
        fetch(group, 0).start()
        fetch(group, 1).start()
    for ref in (acc_ref, zero_ref):
        ref[...] = jnp.zeros_like(ref)
    for j in range(span // LANES):
        part = pl.ds(j * LANES, LANES)
        kpos = lax.broadcasted_iota(jnp.int32, (LANES, tokens), 0) + j * LANES
        qpos = lax.broadcasted_iota(jnp.int32, (LANES, tokens), 1) + (span - tokens)
        seen = (kpos >= starts[...]) & (kpos <= qpos)
        bias_ref[part, :] = jnp.where(seen, 0.0, HIDDEN)
    for slot in range(2):
        for ref in (score_refs, dprob_refs, probs_refs, dscore_refs, top_refs, inverse_refs):
            ref[slot][...] = jnp.zeros_like(ref[slot])
    least = 0
    for size in sizes:
        pl.when((count[0] * LANES > least) & (count[0] * LANES <= size))(functools.partial(run, size))
        least = size
    turned_ref[...] = acc_ref[...].T
    for pair in range(trips - 1):
        put(pair).wait()


def attend(count, starts, rope, q, g, kv):
    heads, depth, tokens = q.shape
    vdim = g.shape[2]
    span, wide = kv.shape[1:]
    sizes = sorted({span // 2, span - 2 * LANES, span - LANES, span})
    smem = pl.BlockSpec(memory_space=pltpu.SMEM)
    vmem = pl.BlockSpec(memory_space=pltpu.VMEM)
    hbm = pl.BlockSpec(memory_space=pl.ANY)
    two = lambda shape, kind: [pltpu.VMEM(shape, kind)] * 2
    return pl.pallas_call(
        functools.partial(attend_kernel, tokens, depth ** (-0.5), sizes),
        in_specs=[smem, vmem, vmem, hbm, hbm, hbm],
        out_specs=[hbm, hbm, vmem],
        out_shape=[
            jax.ShapeDtypeStruct((heads, depth, tokens), BF16),
            jax.ShapeDtypeStruct((heads, span, wide), BF16),
            jax.ShapeDtypeStruct((rope.shape[1], span), F32),
        ],
        scratch_shapes=[
            pltpu.VMEM((heads, depth, tokens), BF16),
            pltpu.VMEM((heads, tokens, vdim), BF16),
            pltpu.VMEM((heads, depth, tokens), BF16),
            pltpu.VMEM((RING, 2, span, wide), BF16),
            pltpu.VMEM((2, 2, span, wide), BF16),
            pltpu.VMEM((MANY, span // 2, wide), BF16),
            pltpu.VMEM((span, tokens), F32),
            pltpu.VMEM(rope.shape, F32),
            two((span, tokens), F32),
            two((span, tokens), F32),
            two((span, tokens), BF16),
            two((span, tokens), BF16),
            two((1, tokens), F32),
            two((1, tokens), F32),
            pltpu.SemaphoreType.DMA((2, heads // MANY)),
            pltpu.SemaphoreType.DMA((RING,)),
            pltpu.SemaphoreType.DMA((2,)),
            pltpu.SemaphoreType.DMA((heads // MANY,)),
            pltpu.SemaphoreType.DMA((heads // 2,)),
        ],
        compiler_params=pltpu.CompilerParams(
            vmem_limit_bytes=60 * 1024 * 1024,
        ),
        name="attend",
    )(count, starts, rope, q, g, kv)


def places():
    me = lax.axis_index("seq")
    count = lax.axis_size("seq")
    head = lax.axis_index("head")
    ahead = [(lax.rem(me + r, count), head) for r in range(1, BACK + 1)]
    behind = [(lax.rem(me + count - r, count), head) for r in range(1, BACK + 1)]
    return head, ahead, behind, (me, 1 - head)


def greet(peers):
    barrier = pltpu.get_barrier_semaphore()
    for peer in peers:
        pl.semaphore_signal(barrier, inc=1, device_id=peer, device_id_type=pl.DeviceIdType.MESH)


def await_all(peers):
    pl.semaphore_wait(pltpu.get_barrier_semaphore(), len(peers))


def meet(peers):
    greet(peers)
    await_all(peers)


def link(src, dst, sems, slot, peer):
    return pltpu.make_async_remote_copy(
        src_ref=src, dst_ref=dst, send_sem=sems.at[0, slot], recv_sem=sems.at[1, slot],
        device_id=peer, device_id_type=pl.DeviceIdType.MESH,
    )


def weights_of(uk_hbm, uv_hbm, uk_ref, uv_ref, sems):
    deep = min(DEEP, uk_ref.shape[0])

    def fetch(group):
        some = pl.ds(group * deep, deep)
        return [
            pltpu.make_async_copy(uk_hbm.at[some], uk_ref.at[some], sems.at[0, group]),
            pltpu.make_async_copy(uv_hbm.at[some], uv_ref.at[some], sems.at[1, group]),
        ]

    return deep, uk_ref.shape[0] // deep, fetch


def project_kernel(remote, own_ref, uk_hbm, uv_hbm, kv_hbm, rope_ref, keys_ref, lat_ref, uk_ref, uv_ref, kv_ref,
                   in_sems, out_sems, *link_sems):
    width = own_ref.shape[0]
    span, rope = rope_ref.shape
    latw, nope = width - rope, uk_ref.shape[2]
    tokens = span // (BACK + 1)
    half = tokens // 2
    deep, groups, fetch = weights_of(uk_hbm, uv_hbm, uk_ref, uv_ref, in_sems)
    for group in range(groups):
        for copy in fetch(group):
            copy.start()

    def out(group, r):
        some, part = pl.ds(group * deep, deep), pl.ds(r * tokens, tokens)
        return pltpu.make_async_copy(kv_ref.at[some, part], kv_hbm.at[some, part], out_sems.at[r, group])

    if remote:
        far_sems, near_sems = link_sems
        head, ahead, behind, sibling = places()
        mine = pl.ds(pl.multiple_of(head * half, half), half)

        def far(r):
            place = BACK - 1 - r
            return link(own_ref.at[:, mine], keys_ref.at[place, :, mine], far_sems, r, ahead[r])

        def near(r):
            landed = keys_ref.at[BACK - 1 - r, :, mine]
            return link(landed, landed, near_sems, r, sibling)

        meet(ahead + behind + [sibling])
        for r in range(BACK):
            far(r).start()

    def block(turn, carry):
        place = BACK - turn
        if remote:
            @pl.when(turn == 0)
            def _():
                lat_ref[...] = own_ref[...].T

            @pl.when(turn == 1)
            def _():
                for r in range(BACK):
                    far(r).wait_recv()
                    near(r).start()

            @pl.when(turn > 0)
            def _():
                near(turn - 1).wait_recv()
                lat_ref[...] = keys_ref[place].T
        else:
            lat_ref[...] = own_ref[:, pl.ds(pl.multiple_of(place * tokens, tokens), tokens)].T
        part = pl.ds(pl.multiple_of(place * tokens, tokens), tokens)
        rope_ref[part, :] = lat_ref[:, latw:]

        def some(group, carry):
            @pl.when(turn == 0)
            def _():
                for copy in fetch(group):
                    copy.wait()

            for i in range(deep):
                index = group * deep + i
                both = jnp.concatenate([uk_ref[index], uv_ref[index]], 1)
                kv_ref[index, part, :] = dot(lat_ref[:, :latw], both).astype(BF16)
            out(group, place).start()
            return carry

        return lax.fori_loop(0, groups, some, carry)

    lax.fori_loop(0, BACK + 1, block, 0)
    if remote:
        for r in range(BACK):
            far(r).wait_send()
            near(r).wait_send()
    for r in range(BACK + 1):
        for group in range(groups):
            out(group, r).wait()


def project(own, uk, uv, span, rope, remote):
    width = own.shape[0]
    tokens = span // (BACK + 1)
    heads, latw, nope = uk.shape
    groups = heads // min(DEEP, heads)
    wide = nope + uv.shape[2]
    vmem = pl.BlockSpec(memory_space=pltpu.VMEM)
    hbm = pl.BlockSpec(memory_space=pl.ANY)
    links = [pltpu.SemaphoreType.DMA((2, BACK))] * 2 if remote else []
    extra = dict(collective_id=0, has_side_effects=True) if remote else {}
    return pl.pallas_call(
        functools.partial(project_kernel, remote),
        in_specs=[vmem, hbm, hbm],
        out_specs=[hbm, vmem],
        out_shape=[
            jax.ShapeDtypeStruct((heads, span, wide), BF16),
            jax.ShapeDtypeStruct((span, rope), BF16),
        ],
        scratch_shapes=[
            pltpu.VMEM((BACK, width, tokens), BF16),
            pltpu.VMEM((tokens, width), BF16),
            pltpu.VMEM(uk.shape, BF16),
            pltpu.VMEM(uv.shape, BF16),
            pltpu.VMEM((heads, span, wide), BF16),
            pltpu.SemaphoreType.DMA((2, groups)),
            pltpu.SemaphoreType.DMA((BACK + 1, groups)),
            *links,
        ],
        compiler_params=pltpu.CompilerParams(vmem_limit_bytes=60 * 1024 * 1024, **extra),
        name="project",
    )(own, uk, uv)


def fold_kernel(remote, dkv_hbm, turned_ref, uk_hbm, uv_hbm, out_ref, uk_ref, uv_ref, dkv_ref, sum_refs, in_sems,
                dkv_sems, *refs):
    rope, span = turned_ref.shape
    latw = uk_ref.shape[1]
    tokens = span // (BACK + 1)
    half = tokens // 2
    deep, groups, fetch = weights_of(uk_hbm, uv_hbm, uk_ref, uv_ref, in_sems)

    def load(group, r):
        some, part = pl.ds(group * deep, deep), pl.ds(r * tokens, tokens)
        return pltpu.make_async_copy(dkv_hbm.at[some, part], dkv_ref.at[some, part], dkv_sems.at[group, r])

    if remote:
        mine_ref, theirs_ref, near_ref, part_ref, far_ref, near_sems, far_sems = refs
        head, ahead, behind, sibling = places()
        peers = ahead + behind + [sibling]
        greet(peers)
    for r in range(BACK + 1):
        for group in range(groups):
            if r == 0:
                for copy in fetch(group):
                    copy.start()
            load(group, r).start()

    def piece(r, group):
        part = pl.ds(pl.multiple_of(r * tokens, tokens), tokens)

        @pl.when(r == 0)
        def _():
            for copy in fetch(group):
                copy.wait()

        load(group, r).wait()
        keep = jnp.where(group == 0, 0.0, 1.0)
        for side in range(2):
            some = [group * deep + side * deep // 2 + i for i in range(deep // 2)]
            left = jnp.concatenate([ref[i] for i in some for ref in (uk_ref, uv_ref)], 1)
            right = jnp.concatenate([dkv_ref[i, part, :] for i in some], 1)
            sum_refs[side][...] = dot(left, right, NT) + keep * sum_refs[side][...]

    for side in range(2):
        sum_refs[side][...] = jnp.zeros_like(sum_refs[side])
    if not remote:
        def plain(r, carry):
            for group in range(groups):
                piece(r, group)
            out_ref[r, :latw, :] = sum_refs[0][...] + sum_refs[1][...]
            out_ref[r, latw:, :] = turned_ref[:, pl.ds(pl.multiple_of(r * tokens, tokens), tokens)]
            return carry

        lax.fori_loop(0, BACK + 1, plain, 0)
        return
    own = pl.ds(pl.multiple_of(head * half, half), half)
    other = pl.ds(pl.multiple_of((1 - head) * half, half), half)
    count = lax.axis_size("seq")
    me = lax.axis_index("seq")

    def near(r):
        return link(theirs_ref.at[r], near_ref.at[r], near_sems, r, sibling)

    def far(r):
        peer = (lax.rem(me + count - BACK + r, count), head)
        return link(part_ref.at[r], far_ref.at[r], far_sems, r, peer)

    await_all(peers)

    def block(r, carry):
        def some(group, carry):
            piece(r, group)

            @pl.when((group == 0) & (r > 0))
            def _():
                near(r - 1).wait_recv()
                part_ref[r - 1] = (mine_ref[r - 1] + near_ref[r - 1].astype(F32)).astype(BF16)
                far(r - 1).start()

            return carry

        lax.fori_loop(0, groups, some, 0)
        theirs_ref[r, :latw, :] = (sum_refs[0][:, other] + sum_refs[1][:, other]).astype(BF16)
        mine_ref[r, :latw, :] = sum_refs[0][:, own] + sum_refs[1][:, own]
        place = [pl.ds(pl.multiple_of(r * tokens + i * half, half), half) for i in (head, 1 - head)]
        theirs_ref[r, latw:, :] = turned_ref[:, place[1]].astype(BF16)
        mine_ref[r, latw:, :] = turned_ref[:, place[0]]
        near(r).start()
        return carry

    lax.fori_loop(0, BACK + 1, block, 0)
    total = mine_ref[BACK]
    for r in range(BACK):
        far(r).wait_recv()
        total += far_ref[r].astype(F32)
    near(BACK).wait_recv()
    out_ref[...] = total + near_ref[BACK].astype(F32)
    for r in range(BACK + 1):
        near(r).wait_send()
    for r in range(BACK):
        far(r).wait_send()


def fold(dkv, turned, uk, uv, remote):
    heads, span, wide = dkv.shape
    rope = turned.shape[0]
    latw = uk.shape[1]
    width = latw + rope
    tokens = span // (BACK + 1)
    half = tokens // 2
    groups = heads // min(DEEP, heads)
    vmem = pl.BlockSpec(memory_space=pltpu.VMEM)
    hbm = pl.BlockSpec(memory_space=pl.ANY)
    links = []
    if remote:
        links = [
            pltpu.VMEM((BACK + 1, width, half), F32),
            pltpu.VMEM((BACK + 1, width, half), BF16),
            pltpu.VMEM((BACK + 1, width, half), BF16),
            pltpu.VMEM((BACK, width, half), BF16),
            pltpu.VMEM((BACK, width, half), BF16),
            pltpu.SemaphoreType.DMA((2, BACK + 1)),
            pltpu.SemaphoreType.DMA((2, BACK)),
        ]
    extra = dict(collective_id=1, has_side_effects=True) if remote else {}
    shape = (width, half) if remote else (BACK + 1, width, tokens)
    return pl.pallas_call(
        functools.partial(fold_kernel, remote),
        in_specs=[hbm, vmem, hbm, hbm],
        out_specs=vmem,
        out_shape=jax.ShapeDtypeStruct(shape, F32),
        scratch_shapes=[
            pltpu.VMEM(uk.shape, BF16),
            pltpu.VMEM(uv.shape, BF16),
            pltpu.VMEM(dkv.shape, BF16),
            [pltpu.VMEM((latw, tokens), F32)] * 2,
            pltpu.SemaphoreType.DMA((2, groups)),
            pltpu.SemaphoreType.DMA((groups, BACK + 1)),
            *links,
        ],
        compiler_params=pltpu.CompilerParams(vmem_limit_bytes=60 * 1024 * 1024, **extra),
        name="fold",
    )(dkv, turned, uk, uv)


def shift(block, axis, distance):
    devices = range(lax.axis_size(axis))
    route = [(i - distance, i) for i in devices if i - distance in devices]
    return lax.ppermute(block, axis, route)


def shards(queries, grad_out, latent, w_uk, w_uv, doc_start):
    tokens, heads, depth = queries.shape
    span = (BACK + 1) * tokens
    rope = latent.shape[1] - w_uk.shape[1]
    own = latent.T
    pairs = lax.axis_size("head") == 2
    if not pairs:
        received = [shift(own, "seq", level) for level in range(BACK, 0, -1)]
        own = jnp.concatenate(received + [own], 1)
    kv, turned = project(own, w_uk, w_uv, span, rope, pairs)
    starts = doc_start - (lax.axis_index("seq") - BACK) * tokens
    count = span // LANES - starts[:1] // LANES
    grad_q, dkv, turned = attend(
        count, starts[None, :], turned, queries.transpose(1, 2, 0), grad_out.transpose(1, 0, 2), kv
    )
    grad_query = grad_q.transpose(2, 0, 1)
    folded = fold(dkv, turned, w_uk, w_uv, pairs)
    if pairs:
        return grad_query, folded.T
    back = [shift(folded[BACK - r].astype(BF16), "seq", -r) for r in range(1, BACK + 1)]
    total = folded[BACK]
    for piece in back:
        total = total + piece.astype(F32)
    return grad_query, lax.psum_scatter(total.T, "head", scatter_dimension=0, tiled=True)


def solution(mesh):
    placed = (
        P("seq", "head", None),
        P("seq", "head", None),
        P("seq", None),
        P("head", None, None),
        P("head", None, None),
        P("seq"),
    )
    return jax.shard_map(
        shards,
        mesh=mesh,
        in_specs=placed,
        out_specs=(P("seq", "head", None), P(("seq", "head"), None)),
        check_vma=False,
    )
```

```python
import functools
import math

import jax
import jax.numpy as jnp
from jax import lax
from jax.experimental import pallas as pl
from jax.experimental.pallas import tpu as pltpu
from jax.sharding import PartitionSpec as P

BACK = 3
LANES = 128
STRIP = 32
DEEP = 16
RING = 4
MANY = 4
HIDDEN = -1e30
F32 = jnp.float32
BF16 = jnp.bfloat16
NN = (((1,), (0,)), ((), ()))
NT = (((1,), (1,)), ((), ()))


def dot(a, b, dims=NN):
    return lax.dot_general(a, b, dims, preferred_element_type=F32)


def attend_kernel(tokens, factor, sizes, count, starts, rope_ref, q_ref, g_ref, kv_hbm,
                  gq_hbm, dkv_hbm, turned_ref, gq_ref, kv_ref, dkv_ref, zero_ref, bias_ref, acc_ref,
                  score_refs, dprob_refs, probs_refs, dscore_refs, top_refs, inverse_refs,
                  kv_sems, dkv_sems, zero_sems, out_sems):
    span, rope = rope_ref.shape
    heads, depth, _ = q_ref.shape
    nope = depth - rope
    trips = heads // 2 + 1
    groups = heads // MANY

    def put(pair):
        some = pl.ds(pair * 2, 2)
        return pltpu.make_async_copy(gq_ref.at[some], gq_hbm.at[some], out_sems.at[pair])

    def run(size):
        rows = slice(span - size, span)
        chunks = [slice(r, r + STRIP) for r in range(span - size, span, STRIP)]

        def load(pair, size=size):
            slot = lax.rem(pair, RING)
            return pltpu.make_async_copy(
                kv_hbm.at[pl.ds(pair * 2, 2), pl.ds(span - size, size)],
                kv_ref.at[slot, :, pl.ds(span - size, size)],
                kv_sems.at[slot],
            )

        def save(pair):
            slot = lax.rem(pair, 2)
            return pltpu.make_async_copy(
                dkv_ref.at[slot, :, pl.ds(0, size)],
                dkv_hbm.at[pl.ds(pair * 2, 2), pl.ds(span - size, size)],
                dkv_sems.at[slot],
            )

        def clear(group):
            return pltpu.make_async_copy(
                zero_ref.at[:, pl.ds(0, span - size)],
                dkv_hbm.at[pl.ds(group * MANY, MANY), pl.ds(0, span - size)],
                zero_sems.at[group],
            )

        def half(trip, slot):
            turn = trip * 2 + slot
            first = jnp.minimum(turn, heads - 1)
            last = jnp.clip(turn - 2, 0, heads - 1)
            now = lax.rem(jnp.minimum(trip, trips - 2), RING)
            before = lax.rem(jnp.maximum(trip - 1, 0), RING)
            probs, dscore = probs_refs[slot], dscore_refs[slot]
            inverse = inverse_refs[slot][...]
            turned = (g_ref[last].T.astype(F32) * inverse).astype(BF16)
            query = (q_ref[last].astype(F32) * (inverse * factor)).astype(BF16)
            dvalue = dot(probs[rows, :], turned, NT)
            dkey = dot(dscore[rows, :], query, NT)
            place = lax.rem(trip + 1, 2)
            dkv_ref[place, slot, :size, nope:] = dvalue.astype(BF16)
            dkv_ref[place, slot, :size, :nope] = dkey[:, :nope].astype(BF16)
            acc_ref[rows, :] += dkey[:, nope:]
            key = jnp.concatenate([kv_ref[now, slot, rows, :nope], rope_ref[rows, :]], 1)
            scores = dot(key, q_ref[first]) + bias_ref[rows, :]
            score_refs[slot][rows, :] = scores
            top_refs[slot][...] = jnp.max(scores, 0, keepdims=True)
            dprob_refs[slot][rows, :] = dot(kv_ref[now, slot, rows, nope:], g_ref[first], NT)
            key = jnp.concatenate([kv_ref[before, slot, rows, :nope], rope_ref[rows, :]], 1)
            dq = dot(key.T, dscore[rows, :])
            gq_ref[last] = (dq * (inverse * factor)).astype(BF16)

        def normalize(slot, turn):
            score_ref, dprob_ref = score_refs[slot], dprob_refs[slot]
            probs_ref, dscore_ref = probs_refs[slot], dscore_refs[slot]
            top = top_refs[slot][...]
            total = jnp.zeros((STRIP, tokens), F32)
            delta = jnp.zeros((STRIP, tokens), F32)
            for part in chunks:
                expo = jnp.exp2((score_ref[part, :] - top) * (factor * math.log2(math.e)))
                probs_ref[part, :] = expo.astype(BF16)
                total += expo
                delta += expo * dprob_ref[part, :]
            inverse = 1.0 / jnp.sum(total, 0, keepdims=True)
            delta = jnp.sum(delta, 0, keepdims=True) * inverse
            valid = jnp.where((turn >= 0) & (turn < heads), 1.0, 0.0)
            inverse_refs[slot][...] = inverse * valid
            for part in chunks:
                expo = probs_ref[part, :].astype(F32)
                dscore_ref[part, :] = (expo * (dprob_ref[part, :] - delta)).astype(BF16)

        def step(trip, carry):
            @pl.when((trip > 0) & (trip < trips - 1))
            def _():
                load(trip).wait()

            @pl.when(trip < trips - 3)
            def _():
                load(trip + 2).start()

            @pl.when(trip > 2)
            def _():
                save(trip - 3).wait()

            half(trip, 0)
            normalize(1, trip * 2 - 1)
            half(trip, 1)
            normalize(0, trip * 2)

            @pl.when(trip > 0)
            def _():
                put(trip - 1).start()
                save(trip - 1).start()

            return carry

        if size < span:
            for group in range(groups):
                clear(group).start()
        load(1).start()
        prime.wait()
        lax.fori_loop(0, trips, step, 0)
        for pair in range(max(trips - 3, 0), trips - 1):
            save(pair).wait()
        if size < span:
            for group in range(groups):
                clear(group).wait()

    prime = pltpu.make_async_copy(kv_hbm.at[pl.ds(0, 2)], kv_ref.at[0], kv_sems.at[0])
    prime.start()
    for ref in (acc_ref, zero_ref):
        ref[...] = jnp.zeros_like(ref)
    for j in range(span // LANES):
        part = pl.ds(j * LANES, LANES)
        kpos = lax.broadcasted_iota(jnp.int32, (LANES, tokens), 0) + j * LANES
        qpos = lax.broadcasted_iota(jnp.int32, (LANES, tokens), 1) + (span - tokens)
        seen = (kpos >= starts[...]) & (kpos <= qpos)
        bias_ref[part, :] = jnp.where(seen, 0.0, HIDDEN)
    for slot in range(2):
        for ref in (score_refs, dprob_refs, probs_refs, dscore_refs, top_refs, inverse_refs):
            ref[slot][...] = jnp.zeros_like(ref[slot])
    least = 0
    for size in sizes:
        pl.when((count[0] * LANES > least) & (count[0] * LANES <= size))(functools.partial(run, size))
        least = size
    turned_ref[...] = acc_ref[...].T
    for pair in range(trips - 1):
        put(pair).wait()


def attend(count, starts, rope, q, g, kv):
    heads, depth, tokens = q.shape
    span, wide = kv.shape[1:]
    sizes = sorted({span // 2, span - 2 * LANES, span - LANES, span})
    smem = pl.BlockSpec(memory_space=pltpu.SMEM)
    vmem = pl.BlockSpec(memory_space=pltpu.VMEM)
    hbm = pl.BlockSpec(memory_space=pl.ANY)
    two = lambda shape, kind: [pltpu.VMEM(shape, kind)] * 2
    return pl.pallas_call(
        functools.partial(attend_kernel, tokens, depth ** (-0.5), sizes),
        in_specs=[smem, vmem, vmem, vmem, vmem, hbm],
        out_specs=[hbm, hbm, vmem],
        out_shape=[
            jax.ShapeDtypeStruct((heads, depth, tokens), BF16),
            jax.ShapeDtypeStruct((heads, span, wide), BF16),
            jax.ShapeDtypeStruct((rope.shape[1], span), F32),
        ],
        scratch_shapes=[
            pltpu.VMEM((heads, depth, tokens), BF16),
            pltpu.VMEM((RING, 2, span, wide), BF16),
            pltpu.VMEM((2, 2, span, wide), BF16),
            pltpu.VMEM((MANY, span // 2, wide), BF16),
            pltpu.VMEM((span, tokens), F32),
            pltpu.VMEM(rope.shape, F32),
            two((span, tokens), F32),
            two((span, tokens), F32),
            two((span, tokens), BF16),
            two((span, tokens), BF16),
            two((1, tokens), F32),
            two((1, tokens), F32),
            pltpu.SemaphoreType.DMA((RING,)),
            pltpu.SemaphoreType.DMA((2,)),
            pltpu.SemaphoreType.DMA((heads // MANY,)),
            pltpu.SemaphoreType.DMA((heads // 2,)),
        ],
        compiler_params=pltpu.CompilerParams(
            vmem_limit_bytes=24 * 1024 * 1024,
        ),
        input_output_aliases={5: 1},
        name="attend",
    )(count, starts, rope, q, g, kv)


def places():
    me = lax.axis_index("seq")
    count = lax.axis_size("seq")
    head = lax.axis_index("head")
    ahead = [(lax.rem(me + r, count), head) for r in range(1, BACK + 1)]
    behind = [(lax.rem(me + count - r, count), head) for r in range(1, BACK + 1)]
    return head, ahead, behind, (me, 1 - head)


def greet(peers):
    barrier = pltpu.get_barrier_semaphore()
    for peer in peers:
        pl.semaphore_signal(barrier, inc=1, device_id=peer, device_id_type=pl.DeviceIdType.MESH)


def await_all(peers):
    pl.semaphore_wait(pltpu.get_barrier_semaphore(), len(peers))


def meet(peers):
    greet(peers)
    await_all(peers)


def link(src, dst, sems, slot, peer):
    return pltpu.make_async_remote_copy(
        src_ref=src, dst_ref=dst, send_sem=sems.at[0, slot], recv_sem=sems.at[1, slot],
        device_id=peer, device_id_type=pl.DeviceIdType.MESH,
    )


def project_kernel(remote, own_ref, uk_ref, uv_ref, kv_ref, rope_ref, keys_ref, lat_ref, *link_sems):
    width = own_ref.shape[0]
    span, rope = rope_ref.shape
    latw, nope = width - rope, uk_ref.shape[2]
    tokens = span // (BACK + 1)
    half = tokens // 2
    deep = min(DEEP, uk_ref.shape[0])
    groups = uk_ref.shape[0] // deep

    if remote:
        far_sems, near_sems = link_sems
        head, ahead, behind, sibling = places()
        mine = pl.ds(pl.multiple_of(head * half, half), half)

        def far(r):
            place = BACK - 1 - r
            return link(own_ref.at[:, mine], keys_ref.at[place, :, mine], far_sems, r, ahead[r])

        def near(r):
            landed = keys_ref.at[BACK - 1 - r, :, mine]
            return link(landed, landed, near_sems, r, sibling)

        meet(ahead + behind + [sibling])
        for r in range(BACK):
            far(r).start()

    def block(turn, carry):
        place = BACK - turn
        if remote:
            @pl.when(turn == 0)
            def _():
                lat_ref[...] = own_ref[...].T

            @pl.when(turn == 1)
            def _():
                for r in range(BACK):
                    far(r).wait_recv()
                    near(r).start()

            @pl.when(turn > 0)
            def _():
                near(turn - 1).wait_recv()
                lat_ref[...] = keys_ref[place].T
        else:
            lat_ref[...] = own_ref[:, pl.ds(pl.multiple_of(place * tokens, tokens), tokens)].T
        part = pl.ds(pl.multiple_of(place * tokens, tokens), tokens)
        rope_ref[part, :] = lat_ref[:, latw:]

        def some(group, carry):
            for i in range(deep):
                index = group * deep + i
                both = jnp.concatenate([uk_ref[index], uv_ref[index]], 1)
                kv_ref[index, part, :] = dot(lat_ref[:, :latw], both).astype(BF16)
            return carry

        return lax.fori_loop(0, groups, some, carry)

    lax.fori_loop(0, BACK + 1, block, 0)
    if remote:
        for r in range(BACK):
            far(r).wait_send()
            near(r).wait_send()


def project(own, uk, uv, span, rope, remote):
    width = own.shape[0]
    tokens = span // (BACK + 1)
    heads, latw, nope = uk.shape
    groups = heads // min(DEEP, heads)
    wide = nope + uv.shape[2]
    vmem = pl.BlockSpec(memory_space=pltpu.VMEM)
    hbm = pl.BlockSpec(memory_space=pl.ANY)
    links = [pltpu.SemaphoreType.DMA((2, BACK))] * 2 if remote else []
    extra = dict(collective_id=0, has_side_effects=True) if remote else {}
    return pl.pallas_call(
        functools.partial(project_kernel, remote),
        in_specs=[vmem, vmem, vmem],
        out_specs=[vmem, vmem],
        out_shape=[
            jax.ShapeDtypeStruct((heads, span, wide), BF16),
            jax.ShapeDtypeStruct((span, rope), BF16),
        ],
        scratch_shapes=[
            pltpu.VMEM((BACK, width, tokens), BF16),
            pltpu.VMEM((tokens, width), BF16),
            *links,
        ],
        compiler_params=pltpu.CompilerParams(vmem_limit_bytes=6 * 1024 * 1024, **extra),
        name="project",
    )(own, uk, uv)


def fold_kernel(remote, dkv_ref, turned_ref, uk_ref, uv_ref, out_ref, sum_refs, *refs):
    rope, span = turned_ref.shape
    latw = uk_ref.shape[1]
    tokens = span // (BACK + 1)
    half = tokens // 2
    deep = min(DEEP, uk_ref.shape[0])
    groups = uk_ref.shape[0] // deep

    if remote:
        mine_ref, theirs_ref, near_ref, part_ref, far_ref, near_sems, far_sems = refs
        head, ahead, behind, sibling = places()
        peers = ahead + behind + [sibling]
        greet(peers)

    def piece(r, group):
        part = pl.ds(pl.multiple_of(r * tokens, tokens), tokens)

        keep = jnp.where(group == 0, 0.0, 1.0)
        for side in range(2):
            some = [group * deep + side * deep // 2 + i for i in range(deep // 2)]
            left = jnp.concatenate([ref[i] for i in some for ref in (uk_ref, uv_ref)], 1)
            right = jnp.concatenate([dkv_ref[i, part, :] for i in some], 1)
            sum_refs[side][...] = dot(left, right, NT) + keep * sum_refs[side][...]

    for side in range(2):
        sum_refs[side][...] = jnp.zeros_like(sum_refs[side])
    if not remote:
        def plain(r, carry):
            for group in range(groups):
                piece(r, group)
            out_ref[r, :latw, :] = sum_refs[0][...] + sum_refs[1][...]
            out_ref[r, latw:, :] = turned_ref[:, pl.ds(pl.multiple_of(r * tokens, tokens), tokens)]
            return carry

        lax.fori_loop(0, BACK + 1, plain, 0)
        return
    own = pl.ds(pl.multiple_of(head * half, half), half)
    other = pl.ds(pl.multiple_of((1 - head) * half, half), half)
    count = lax.axis_size("seq")
    me = lax.axis_index("seq")

    def near(r):
        return link(theirs_ref.at[r], near_ref.at[r], near_sems, r, sibling)

    def far(r):
        peer = (lax.rem(me + count - BACK + r, count), head)
        return link(part_ref.at[r], far_ref.at[r], far_sems, r, peer)

    await_all(peers)

    def block(r, carry):
        def some(group, carry):
            piece(r, group)

            @pl.when((group == 0) & (r > 0))
            def _():
                near(r - 1).wait_recv()
                part_ref[r - 1] = (mine_ref[r - 1] + near_ref[r - 1].astype(F32)).astype(BF16)
                far(r - 1).start()

            return carry

        lax.fori_loop(0, groups, some, 0)
        theirs_ref[r, :latw, :] = (sum_refs[0][:, other] + sum_refs[1][:, other]).astype(BF16)
        mine_ref[r, :latw, :] = sum_refs[0][:, own] + sum_refs[1][:, own]
        place = [pl.ds(pl.multiple_of(r * tokens + i * half, half), half) for i in (head, 1 - head)]
        theirs_ref[r, latw:, :] = turned_ref[:, place[1]].astype(BF16)
        mine_ref[r, latw:, :] = turned_ref[:, place[0]]
        near(r).start()
        return carry

    lax.fori_loop(0, BACK + 1, block, 0)
    total = mine_ref[BACK]
    for r in range(BACK):
        far(r).wait_recv()
        total += far_ref[r].astype(F32)
    near(BACK).wait_recv()
    out_ref[...] = total + near_ref[BACK].astype(F32)
    for r in range(BACK + 1):
        near(r).wait_send()
    for r in range(BACK):
        far(r).wait_send()


def fold(dkv, turned, uk, uv, remote):
    heads, span, wide = dkv.shape
    rope = turned.shape[0]
    latw = uk.shape[1]
    width = latw + rope
    tokens = span // (BACK + 1)
    half = tokens // 2
    groups = heads // min(DEEP, heads)
    vmem = pl.BlockSpec(memory_space=pltpu.VMEM)
    hbm = pl.BlockSpec(memory_space=pl.ANY)
    links = []
    if remote:
        links = [
            pltpu.VMEM((BACK + 1, width, half), F32),
            pltpu.VMEM((BACK + 1, width, half), BF16),
            pltpu.VMEM((BACK + 1, width, half), BF16),
            pltpu.VMEM((BACK, width, half), BF16),
            pltpu.VMEM((BACK, width, half), BF16),
            pltpu.SemaphoreType.DMA((2, BACK + 1)),
            pltpu.SemaphoreType.DMA((2, BACK)),
        ]
    extra = dict(collective_id=1, has_side_effects=True) if remote else {}
    shape = (width, half) if remote else (BACK + 1, width, tokens)
    return pl.pallas_call(
        functools.partial(fold_kernel, remote),
        in_specs=[vmem, vmem, vmem, vmem],
        out_specs=vmem,
        out_shape=jax.ShapeDtypeStruct(shape, F32),
        scratch_shapes=[
            [pltpu.VMEM((latw, tokens), F32)] * 2,
            *links,
        ],
        compiler_params=pltpu.CompilerParams(vmem_limit_bytes=8 * 1024 * 1024, **extra),
        name="fold",
    )(dkv, turned, uk, uv)


def shift(block, axis, distance):
    devices = range(lax.axis_size(axis))
    route = [(i - distance, i) for i in devices if i - distance in devices]
    return lax.ppermute(block, axis, route)


def shards(queries, grad_out, latent, w_uk, w_uv, doc_start):
    tokens, heads, depth = queries.shape
    span = (BACK + 1) * tokens
    rope = latent.shape[1] - w_uk.shape[1]
    own = latent.T
    pairs = lax.axis_size("head") == 2
    if not pairs:
        received = [shift(own, "seq", level) for level in range(BACK, 0, -1)]
        own = jnp.concatenate(received + [own], 1)
    kv, turned = project(own, w_uk, w_uv, span, rope, pairs)
    starts = doc_start - (lax.axis_index("seq") - BACK) * tokens
    count = span // LANES - starts[:1] // LANES
    grad_q, dkv, turned = attend(
        count, starts[None, :], turned, queries.transpose(1, 2, 0), grad_out.transpose(1, 0, 2), kv
    )
    grad_query = grad_q.transpose(2, 0, 1)
    folded = fold(dkv, turned, w_uk, w_uv, pairs)
    if pairs:
        return grad_query, folded.T
    back = [shift(folded[BACK - r].astype(BF16), "seq", -r) for r in range(1, BACK + 1)]
    total = folded[BACK]
    for piece in back:
        total = total + piece.astype(F32)
    return grad_query, lax.psum_scatter(total.T, "head", scatter_dimension=0, tiled=True)


def solution(mesh):
    placed = (
        P("seq", "head", None),
        P("seq", "head", None),
        P("seq", None),
        P("head", None, None),
        P("head", None, None),
        P("seq"),
    )
    return jax.shard_map(
        shards,
        mesh=mesh,
        in_specs=placed,
        out_specs=(P("seq", "head", None), P(("seq", "head"), None)),
        check_vma=False,
    )
```

```python
import functools
import math

import jax
import jax.numpy as jnp
from jax import lax
from jax.experimental import pallas as pl
from jax.experimental.pallas import tpu as pltpu
from jax.sharding import PartitionSpec as P

BACK = 3
LANES = 128
STRIP = 32
DEEP = 16
RING = 4
MANY = 4
HIDDEN = -1e30
F32 = jnp.float32
BF16 = jnp.bfloat16
NN = (((1,), (0,)), ((), ()))
NT = (((1,), (1,)), ((), ()))


def dot(a, b, dims=NN):
    return lax.dot_general(a, b, dims, preferred_element_type=F32)


def attend_kernel(tokens, factor, sizes, count, starts, rope_ref, q_ref, g_ref, kv_hbm,
                  gq_hbm, dkv_hbm, turned_ref, gq_ref, kv_ref, dkv_ref, zero_ref, bias_ref, acc_ref,
                  score_refs, dprob_refs, probs_refs, dscore_refs, top_refs, inverse_refs,
                  kv_sems, dkv_sems, zero_sems, out_sems):
    span, rope = rope_ref.shape
    heads, depth, _ = q_ref.shape
    nope = depth - rope
    trips = heads // 2 + 1
    groups = heads // MANY

    def put(pair):
        some = pl.ds(pair * 2, 2)
        return pltpu.make_async_copy(gq_ref.at[some], gq_hbm.at[some], out_sems.at[pair])

    def run(size):
        rows = slice(span - size, span)
        chunks = [slice(r, r + STRIP) for r in range(span - size, span, STRIP)]

        def load(pair, size=size):
            slot = lax.rem(pair, RING)
            return pltpu.make_async_copy(
                kv_hbm.at[pl.ds(pair * 2, 2), pl.ds(span - size, size)],
                kv_ref.at[slot, :, pl.ds(span - size, size)],
                kv_sems.at[slot],
            )

        def save(pair):
            slot = lax.rem(pair, 2)
            return pltpu.make_async_copy(
                dkv_ref.at[slot, :, pl.ds(0, size)],
                dkv_hbm.at[pl.ds(pair * 2, 2), pl.ds(span - size, size)],
                dkv_sems.at[slot],
            )

        def clear(group):
            return pltpu.make_async_copy(
                zero_ref.at[:, pl.ds(0, span - size)],
                dkv_hbm.at[pl.ds(group * MANY, MANY), pl.ds(0, span - size)],
                zero_sems.at[group],
            )

        def half(trip, slot):
            turn = trip * 2 + slot
            first = jnp.minimum(turn, heads - 1)
            last = jnp.clip(turn - 2, 0, heads - 1)
            now = lax.rem(jnp.minimum(trip, trips - 2), RING)
            before = lax.rem(jnp.maximum(trip - 1, 0), RING)
            probs, dscore = probs_refs[slot], dscore_refs[slot]
            inverse = inverse_refs[slot][...]
            turned = (g_ref[last].T.astype(F32) * inverse).astype(BF16)
            query = (q_ref[last].astype(F32) * (inverse * factor)).astype(BF16)
            dvalue = dot(probs[rows, :], turned, NT)
            dkey = dot(dscore[rows, :], query, NT)
            place = lax.rem(trip + 1, 2)
            dkv_ref[place, slot, :size, nope:] = dvalue.astype(BF16)
            dkv_ref[place, slot, :size, :nope] = dkey[:, :nope].astype(BF16)
            acc_ref[rows, :] += dkey[:, nope:]
            key = jnp.concatenate([kv_ref[now, slot, rows, :nope], rope_ref[rows, :]], 1)
            scores = dot(key, q_ref[first]) + bias_ref[rows, :]
            score_refs[slot][rows, :] = scores
            top_refs[slot][...] = jnp.max(scores, 0, keepdims=True)
            dprob_refs[slot][rows, :] = dot(kv_ref[now, slot, rows, nope:], g_ref[first], NT)
            key = jnp.concatenate([kv_ref[before, slot, rows, :nope], rope_ref[rows, :]], 1)
            dq = dot(key.T, dscore[rows, :])
            gq_ref[last] = (dq * (inverse * factor)).astype(BF16)

        def normalize(slot, turn):
            score_ref, dprob_ref = score_refs[slot], dprob_refs[slot]
            probs_ref, dscore_ref = probs_refs[slot], dscore_refs[slot]
            top = top_refs[slot][...]
            total = jnp.zeros((STRIP, tokens), F32)
            delta = jnp.zeros((STRIP, tokens), F32)
            for part in chunks:
                expo = jnp.exp2((score_ref[part, :] - top) * (factor * math.log2(math.e)))
                probs_ref[part, :] = expo.astype(BF16)
                total += expo
                delta += expo * dprob_ref[part, :]
            inverse = 1.0 / jnp.sum(total, 0, keepdims=True)
            delta = jnp.sum(delta, 0, keepdims=True) * inverse
            valid = jnp.where((turn >= 0) & (turn < heads), 1.0, 0.0)
            inverse_refs[slot][...] = inverse * valid
            for part in chunks:
                expo = probs_ref[part, :].astype(F32)
                dscore_ref[part, :] = (expo * (dprob_ref[part, :] - delta)).astype(BF16)

        def step(trip, carry):
            @pl.when((trip > 0) & (trip < trips - 1))
            def _():
                load(trip).wait()

            @pl.when(trip < trips - 3)
            def _():
                load(trip + 2).start()

            @pl.when(trip > 2)
            def _():
                save(trip - 3).wait()

            half(trip, 0)
            normalize(1, trip * 2 - 1)
            half(trip, 1)
            normalize(0, trip * 2)

            @pl.when(trip > 0)
            def _():
                put(trip - 1).start()
                save(trip - 1).start()

            return carry

        if size < span:
            for group in range(groups):
                clear(group).start()
        load(1).start()
        prime.wait()
        lax.fori_loop(0, trips, step, 0)
        for pair in range(max(trips - 3, 0), trips - 1):
            save(pair).wait()
        if size < span:
            for group in range(groups):
                clear(group).wait()

    prime = pltpu.make_async_copy(kv_hbm.at[pl.ds(0, 2)], kv_ref.at[0], kv_sems.at[0])
    prime.start()
    for ref in (acc_ref, zero_ref):
        ref[...] = jnp.zeros_like(ref)
    for j in range(span // LANES):
        part = pl.ds(j * LANES, LANES)
        kpos = lax.broadcasted_iota(jnp.int32, (LANES, tokens), 0) + j * LANES
        qpos = lax.broadcasted_iota(jnp.int32, (LANES, tokens), 1) + (span - tokens)
        seen = (kpos >= starts[...]) & (kpos <= qpos)
        bias_ref[part, :] = jnp.where(seen, 0.0, HIDDEN)
    for slot in range(2):
        for ref in (score_refs, dprob_refs, probs_refs, dscore_refs, top_refs, inverse_refs):
            ref[slot][...] = jnp.zeros_like(ref[slot])
    least = 0
    for size in sizes:
        pl.when((count[0] * LANES > least) & (count[0] * LANES <= size))(functools.partial(run, size))
        least = size
    turned_ref[...] = acc_ref[...].T
    for pair in range(trips - 1):
        put(pair).wait()


def attend(count, starts, rope, q, g, kv):
    heads, depth, tokens = q.shape
    span, wide = kv.shape[1:]
    sizes = sorted({span // 2, span - 2 * LANES, span - LANES, span})
    smem = pl.BlockSpec(memory_space=pltpu.SMEM)
    vmem = pl.BlockSpec(memory_space=pltpu.VMEM)
    hbm = pl.BlockSpec(memory_space=pl.ANY)
    two = lambda shape, kind: [pltpu.VMEM(shape, kind)] * 2
    return pl.pallas_call(
        functools.partial(attend_kernel, tokens, depth ** (-0.5), sizes),
        in_specs=[smem, vmem, vmem, vmem, vmem, hbm],
        out_specs=[hbm, hbm, vmem],
        out_shape=[
            jax.ShapeDtypeStruct((heads, depth, tokens), BF16),
            jax.ShapeDtypeStruct((heads, span, wide), BF16),
            jax.ShapeDtypeStruct((rope.shape[1], span), F32),
        ],
        scratch_shapes=[
            pltpu.VMEM((heads, depth, tokens), BF16),
            pltpu.VMEM((RING, 2, span, wide), BF16),
            pltpu.VMEM((2, 2, span, wide), BF16),
            pltpu.VMEM((MANY, span // 2, wide), BF16),
            pltpu.VMEM((span, tokens), F32),
            pltpu.VMEM(rope.shape, F32),
            two((span, tokens), F32),
            two((span, tokens), F32),
            two((span, tokens), BF16),
            two((span, tokens), BF16),
            two((1, tokens), F32),
            two((1, tokens), F32),
            pltpu.SemaphoreType.DMA((RING,)),
            pltpu.SemaphoreType.DMA((2,)),
            pltpu.SemaphoreType.DMA((heads // MANY,)),
            pltpu.SemaphoreType.DMA((heads // 2,)),
        ],
        compiler_params=pltpu.CompilerParams(
            vmem_limit_bytes=24 * 1024 * 1024,
        ),
        input_output_aliases={5: 1},
        name="attend",
    )(count, starts, rope, q, g, kv)


def places():
    me = lax.axis_index("seq")
    count = lax.axis_size("seq")
    head = lax.axis_index("head")
    ahead = [(lax.rem(me + r, count), head) for r in range(1, BACK + 1)]
    behind = [(lax.rem(me + count - r, count), head) for r in range(1, BACK + 1)]
    return head, ahead, behind, (me, 1 - head)


def greet(peers):
    barrier = pltpu.get_barrier_semaphore()
    for peer in peers:
        pl.semaphore_signal(barrier, inc=1, device_id=peer, device_id_type=pl.DeviceIdType.MESH)


def await_all(peers):
    pl.semaphore_wait(pltpu.get_barrier_semaphore(), len(peers))


def meet(peers):
    greet(peers)
    await_all(peers)


def link(src, dst, sems, slot, peer):
    return pltpu.make_async_remote_copy(
        src_ref=src, dst_ref=dst, send_sem=sems.at[0, slot], recv_sem=sems.at[1, slot],
        device_id=peer, device_id_type=pl.DeviceIdType.MESH,
    )


def project_kernel(remote, own_hbm, uk_ref, uv_hbm, kv_ref, rope_ref, own_ref, uv_ref, keys_ref, lat_ref, in_sems,
                   *link_sems):
    width = own_ref.shape[0]
    early = pltpu.make_async_copy(own_hbm, own_ref, in_sems.at[0])
    early.start()
    weights = pltpu.make_async_copy(uv_hbm, uv_ref, in_sems.at[1])
    weights.start()
    span, rope = rope_ref.shape
    latw, nope = width - rope, uk_ref.shape[2]
    tokens = span // (BACK + 1)
    half = tokens // 2
    deep = min(DEEP, uk_ref.shape[0])
    groups = uk_ref.shape[0] // deep

    if remote:
        far_sems, near_sems = link_sems
        head, ahead, behind, sibling = places()
        me, count = lax.axis_index("seq"), lax.axis_size("seq")
        mine = pl.ds(pl.multiple_of(head * half, half), half)

        def far(r):
            place = BACK - 1 - r
            return link(own_ref.at[:, mine], keys_ref.at[place, :, mine], far_sems, r, (lax.rem(me + 1 + r, count), head))

        def near(r):
            landed = keys_ref.at[BACK - 1 - r, :, mine]
            return link(landed, landed, near_sems, r, sibling)

        greet(ahead + behind + [sibling])
        early.wait()
        await_all(ahead + behind + [sibling])
        for r in range(BACK):
            far(r).start()
    else:
        early.wait()

    def forward(r):
        far(r).wait_recv()
        near(r).start()

    def block(turn, carry):
        place = BACK - turn
        if remote:
            @pl.when(turn == 0)
            def _():
                lat_ref[...] = own_ref[...].T
                weights.wait()

            @pl.when(turn == 1)
            def _():
                forward(0)

            @pl.when(turn > 0)
            def _():
                near(turn - 1).wait_recv()
                lat_ref[...] = keys_ref[place].T
        else:
            @pl.when(turn == 0)
            def _():
                weights.wait()

            lat_ref[...] = own_ref[:, pl.ds(pl.multiple_of(place * tokens, tokens), tokens)].T
        part = pl.ds(pl.multiple_of(place * tokens, tokens), tokens)
        rope_ref[part, :] = lat_ref[:, latw:]

        def some(group, carry):
            if remote:
                @pl.when((group == groups - 1) & (turn > 0) & (turn < BACK))
                def _():
                    forward(turn)

            for i in range(deep):
                index = group * deep + i
                both = jnp.concatenate([uk_ref[index], uv_ref[index]], 1)
                kv_ref[index, part, :] = dot(lat_ref[:, :latw], both).astype(BF16)
            return carry

        return lax.fori_loop(0, groups, some, carry)

    lax.fori_loop(0, BACK + 1, block, 0)
    if remote:
        for r in range(BACK):
            far(r).wait_send()
            near(r).wait_send()


def project(own, uk, uv, span, rope, remote):
    width = own.shape[0]
    tokens = span // (BACK + 1)
    heads, latw, nope = uk.shape
    groups = heads // min(DEEP, heads)
    wide = nope + uv.shape[2]
    vmem = pl.BlockSpec(memory_space=pltpu.VMEM)
    hbm = pl.BlockSpec(memory_space=pl.ANY)
    links = [pltpu.SemaphoreType.DMA((2, BACK))] * 2 if remote else []
    extra = dict(collective_id=0, has_side_effects=True) if remote else {}
    return pl.pallas_call(
        functools.partial(project_kernel, remote),
        in_specs=[pl.BlockSpec(memory_space=pltpu.HBM), vmem, pl.BlockSpec(memory_space=pltpu.HBM)],
        out_specs=[vmem, vmem],
        out_shape=[
            jax.ShapeDtypeStruct((heads, span, wide), BF16),
            jax.ShapeDtypeStruct((span, rope), BF16),
        ],
        scratch_shapes=[
            pltpu.VMEM(own.shape, BF16),
            pltpu.VMEM(uv.shape, BF16),
            pltpu.VMEM((BACK, width, tokens), BF16),
            pltpu.VMEM((tokens, width), BF16),
            pltpu.SemaphoreType.DMA((2,)),
            *links,
        ],
        compiler_params=pltpu.CompilerParams(vmem_limit_bytes=11 * 1024 * 1024, **extra),
        name="project",
    )(own, uk, uv)


def fold_kernel(remote, dkv_ref, turned_ref, uk_ref, uv_ref, out_ref, sum_refs, *refs):
    rope, span = turned_ref.shape
    latw = uk_ref.shape[1]
    tokens = span // (BACK + 1)
    half = tokens // 2
    deep = min(DEEP, uk_ref.shape[0])
    groups = uk_ref.shape[0] // deep

    if remote:
        mine_ref, theirs_ref, near_ref, part_ref, far_ref, near_sems, far_sems = refs
        head, ahead, behind, sibling = places()
        peers = ahead + behind + [sibling]
        greet(peers)

    def piece(r, group):
        part = pl.ds(pl.multiple_of(r * tokens, tokens), tokens)

        keep = jnp.where(group == 0, 0.0, 1.0)
        for side in range(2):
            some = [group * deep + side * deep // 2 + i for i in range(deep // 2)]
            left = jnp.concatenate([ref[i] for i in some for ref in (uk_ref, uv_ref)], 1)
            right = jnp.concatenate([dkv_ref[i, part, :] for i in some], 1)
            sum_refs[side][...] = dot(left, right, NT) + keep * sum_refs[side][...]

    for side in range(2):
        sum_refs[side][...] = jnp.zeros_like(sum_refs[side])
    if not remote:
        def plain(r, carry):
            for group in range(groups):
                piece(r, group)
            out_ref[r, :latw, :] = sum_refs[0][...] + sum_refs[1][...]
            out_ref[r, latw:, :] = turned_ref[:, pl.ds(pl.multiple_of(r * tokens, tokens), tokens)]
            return carry

        lax.fori_loop(0, BACK + 1, plain, 0)
        return
    own = pl.ds(pl.multiple_of(head * half, half), half)
    other = pl.ds(pl.multiple_of((1 - head) * half, half), half)
    count = lax.axis_size("seq")
    me = lax.axis_index("seq")

    def near(r):
        return link(theirs_ref.at[r], near_ref.at[r], near_sems, r, sibling)

    def far(r):
        peer = (lax.rem(me + count - BACK + r, count), head)
        return link(part_ref.at[r], far_ref.at[r], far_sems, r, peer)

    await_all(peers)

    def block(r, carry):
        def some(group, carry):
            piece(r, group)

            @pl.when((group == 0) & (r > 0))
            def _():
                near(r - 1).wait_recv()
                part_ref[r - 1] = (mine_ref[r - 1] + near_ref[r - 1].astype(F32)).astype(BF16)
                far(r - 1).start()

            return carry

        lax.fori_loop(0, groups, some, 0)
        theirs_ref[r, :latw, :] = (sum_refs[0][:, other] + sum_refs[1][:, other]).astype(BF16)
        mine_ref[r, :latw, :] = sum_refs[0][:, own] + sum_refs[1][:, own]
        place = [pl.ds(pl.multiple_of(r * tokens + i * half, half), half) for i in (head, 1 - head)]
        theirs_ref[r, latw:, :] = turned_ref[:, place[1]].astype(BF16)
        mine_ref[r, latw:, :] = turned_ref[:, place[0]]
        near(r).start()
        return carry

    lax.fori_loop(0, BACK + 1, block, 0)
    total = mine_ref[BACK]
    for r in range(BACK):
        far(r).wait_recv()
        total += far_ref[r].astype(F32)
    near(BACK).wait_recv()
    out_ref[...] = total + near_ref[BACK].astype(F32)
    for r in range(BACK + 1):
        near(r).wait_send()
    for r in range(BACK):
        far(r).wait_send()


def fold(dkv, turned, uk, uv, remote):
    heads, span, wide = dkv.shape
    rope = turned.shape[0]
    latw = uk.shape[1]
    width = latw + rope
    tokens = span // (BACK + 1)
    half = tokens // 2
    groups = heads // min(DEEP, heads)
    vmem = pl.BlockSpec(memory_space=pltpu.VMEM)
    hbm = pl.BlockSpec(memory_space=pl.ANY)
    links = []
    if remote:
        links = [
            pltpu.VMEM((BACK + 1, width, half), F32),
            pltpu.VMEM((BACK + 1, width, half), BF16),
            pltpu.VMEM((BACK + 1, width, half), BF16),
            pltpu.VMEM((BACK, width, half), BF16),
            pltpu.VMEM((BACK, width, half), BF16),
            pltpu.SemaphoreType.DMA((2, BACK + 1)),
            pltpu.SemaphoreType.DMA((2, BACK)),
        ]
    extra = dict(collective_id=1, has_side_effects=True) if remote else {}
    shape = (width, half) if remote else (BACK + 1, width, tokens)
    return pl.pallas_call(
        functools.partial(fold_kernel, remote),
        in_specs=[vmem, vmem, vmem, vmem],
        out_specs=vmem,
        out_shape=jax.ShapeDtypeStruct(shape, F32),
        scratch_shapes=[
            [pltpu.VMEM((latw, tokens), F32)] * 2,
            *links,
        ],
        compiler_params=pltpu.CompilerParams(vmem_limit_bytes=8 * 1024 * 1024, **extra),
        name="fold",
    )(dkv, turned, uk, uv)


def shift(block, axis, distance):
    devices = range(lax.axis_size(axis))
    route = [(i - distance, i) for i in devices if i - distance in devices]
    return lax.ppermute(block, axis, route)


def shards(queries, grad_out, latent, w_uk, w_uv, doc_start):
    tokens, heads, depth = queries.shape
    span = (BACK + 1) * tokens
    rope = latent.shape[1] - w_uk.shape[1]
    own = latent.T
    pairs = lax.axis_size("head") == 2
    if not pairs:
        received = [shift(own, "seq", level) for level in range(BACK, 0, -1)]
        own = jnp.concatenate(received + [own], 1)
    kv, turned = project(own, w_uk, w_uv, span, rope, pairs)
    starts = doc_start - (lax.axis_index("seq") - BACK) * tokens
    count = span // LANES - starts[:1] // LANES
    grad_q, dkv, turned = attend(
        count, starts[None, :], turned, queries.transpose(1, 2, 0), grad_out.transpose(1, 0, 2), kv
    )
    grad_query = grad_q.transpose(2, 0, 1)
    folded = fold(dkv, turned, w_uk, w_uv, pairs)
    if pairs:
        return grad_query, folded.T
    back = [shift(folded[BACK - r].astype(BF16), "seq", -r) for r in range(1, BACK + 1)]
    total = folded[BACK]
    for piece in back:
        total = total + piece.astype(F32)
    return grad_query, lax.psum_scatter(total.T, "head", scatter_dimension=0, tiled=True)


def solution(mesh):
    placed = (
        P("seq", "head", None),
        P("seq", "head", None),
        P("seq", None),
        P("head", None, None),
        P("head", None, None),
        P("seq"),
    )
    return jax.shard_map(
        shards,
        mesh=mesh,
        in_specs=placed,
        out_specs=(P("seq", "head", None), P(("seq", "head"), None)),
        check_vma=False,
    )
```
